32 devices in a mesh: grp: 2 (over x), blk: 8 (over z, y), vec: 2 (over core).
Axes of the slice: x: 2, y: 2, z: 4, core: 2. Of those that a mesh axis runs over, the one named last changes fastest.
Arguments:
- trial: bfloat16 [20480, 32], P(('grp', 'blk', 'vec')), may hold values from -6 to 6
- energy_gap: float32 [20480], P(('grp', 'blk', 'vec')), may hold values from 0.5 to 2.5
- coulomb_factors: bfloat16 [4096, 20480], P('blk'), may hold values from -0.0390625 to 0.0390625
- occ_values: bfloat16 [80, 40, 512], P('blk'), may hold values from -1 to 1
- vir_values: bfloat16 [80, 512, 512], P('blk'), may hold values from -1 to 1
- kernel: float32 [80, 512], P('blk'), may hold values from 0.2 to 2
- live_points: int32 [80], P('blk'), may hold values from 64 to 512
Outputs:
- sigma: bfloat16 [20480, 32], P(('grp', 'blk', 'vec'))
The draws below stay inside these ranges and needn't reach their ends.
All inputs are finite; a program needn't handle non-finite values.
Results may differ from the reference program's by a relative error of at most 0.0029.
Values may be sent and summed in bfloat16 or wider, within the bound.
A program may use at most 64 MiB of HBM per device.

```python
import math
import jax
import jax.numpy as jnp
from jax import lax

NOCC = 40
NVIR = 512
NAUX = 4096
K = 32
BATCH = 512
BATCHES = 80
POINTS = 40960
PAIRS = 20480


def touch_ends(values, stream_key, smallest, top_value):
    place = [jax.random.randint(jax.random.fold_in(stream_key, axis), (), 0, length) for axis, length in enumerate(values.shape)]
    widest = values.shape.index(max(values.shape))
    next_to = place[:widest] + [(place[widest] + 1) % values.shape[widest]] + place[widest + 1:]
    return values.at[tuple(place)].set(smallest).at[tuple(next_to)].set(top_value)


def steps_of(own_key, shape, split, smallest, top_value):
    gain, own = 1.0, jax.random.fold_in(own_key, 6)
    for dim, parts in split:
        heights = jnp.exp(jax.random.uniform(jax.random.fold_in(own, dim), (parts,), jnp.float32, smallest / len(split), top_value / len(split)))
        gain = gain * jnp.repeat(heights, shape[dim] // parts).reshape([-1 if axis == dim else 1 for axis in range(len(shape))])
    return gain


def centred(stream_key, dims, spread, reach, shards=(), kind=jnp.bfloat16):
    values = jax.random.normal(stream_key, dims, jnp.float32) * spread
    if len(shards) > 0:
        values = steps_of(stream_key, dims, shards, -0.22, 0.18) * values
    return jnp.clip(values, min=-reach, max=reach).astype(kind)


def setup_inputs(seed: int = 0) -> dict:
    keys = jax.random.split(jax.random.key(seed), 8)
    trial = centred(keys[0], (PAIRS, K), 1.0, 6.0, ((0, 32),))
    energy_gap = jnp.clip(0.5 + 2.0 * jax.random.uniform(keys[1], (PAIRS,), jnp.float32) ** steps_of(keys[1], (PAIRS,), ((0, 32),), -0.2, 0.2), 0.5, 2.5)
    coulomb_factors = centred(keys[2], (NAUX, PAIRS), (NAUX + PAIRS) ** -0.5, 0.0390625, ((0, 8),))
    occ_values = centred(keys[3], (BATCHES, NOCC, BATCH), ((POINTS * PAIRS) ** -0.125), 1.0, ((0, 8),))
    vir_values = centred(keys[4], (BATCHES, BATCH, NVIR), ((POINTS * PAIRS) ** -0.125), 1.0, ((0, 8),))
    kernel = jnp.clip(jnp.exp(math.log(2.0) - 2.3025851 * jax.random.uniform(keys[5], (BATCHES, BATCH), jnp.float32) ** steps_of(keys[5], (BATCHES, BATCH), ((0, 8),), -0.2, 0.2)), 0.2, 2.0)
    live_points = touch_ends(jax.random.randint(keys[6], (BATCHES,), BATCH // 8, BATCH + 1), jax.random.fold_in(keys[6], 1), BATCH // 8, BATCH).astype(jnp.int32)
    return {"trial": trial, "energy_gap": energy_gap, "coulomb_factors": coulomb_factors, "occ_values": occ_values, "vir_values": vir_values, "kernel": kernel, "live_points": live_points}


def reference(trial, energy_gap, coulomb_factors, occ_values, vir_values, kernel, live_points):
    factored = jnp.dot(coulomb_factors, trial, preferred_element_type=jnp.float32).astype(jnp.bfloat16)
    coulomb = 2.0 * lax.dot_general(coulomb_factors, factored, (((0,), (0,)), ((), ())), preferred_element_type=jnp.float32)
    width = trial.shape[1]
    rearranged = trial.reshape(NOCC, NVIR, width).transpose(1, 0, 2).reshape(NVIR, NOCC * width)
    slots = jnp.arange(BATCH, dtype=jnp.int32)

    def step(carry, items):
        occ, vir, weight, live = items
        trans = jnp.dot(vir, rearranged, preferred_element_type=jnp.float32).reshape(BATCH, NOCC, width)
        occ_float = occ.astype(jnp.float32)
        density = jnp.einsum("gik,ig->gk", trans, occ_float)
        mask = (slots < live).astype(jnp.float32)
        weighted = density * (weight * mask)[:, None]
        scaled = (occ_float.T[:, :, None] * weighted[:, None, :]).reshape(BATCH, NOCC * width).astype(jnp.bfloat16)
        return carry + lax.dot_general(vir, scaled, (((0,), (0,)), ((), ())), preferred_element_type=jnp.float32), None

    start = jnp.zeros((NVIR, NOCC * width), jnp.float32)
    total, _ = lax.scan(step, start, (occ_values, vir_values, kernel, live_points))
    exchange = total.reshape(NVIR, NOCC, width).transpose(1, 0, 2).reshape(NOCC * NVIR, width)
    result = energy_gap[:, None] * trial.astype(jnp.float32) + coulomb + exchange
    return result.astype(jnp.bfloat16)
```

```python
import functools

import jax
import jax.numpy as jnp
from jax import lax
from jax.experimental import pallas as pl
from jax.experimental.pallas import tpu as pltpu
from jax.sharding import PartitionSpec as P

LANES = 128
MESH = pl.DeviceIdType.MESH


def collective_local(
    trial, energy_gap, coulomb_factors, occ_values, vir_values, kernel, live_points
):
    pair_rows = lax.all_to_all(trial, "vec", split_axis=1, concat_axis=0, tiled=True)
    full = lax.all_gather(pair_rows, ("grp", "blk"), axis=0, tiled=True)
    occ_count = occ_values.shape[1]
    batch_size = occ_values.shape[2]
    vir_count = vir_values.shape[2]
    width = full.shape[1]
    batches = occ_values.shape[0]
    rearranged = (
        full.reshape(occ_count, vir_count, width)
        .transpose(1, 0, 2)
        .reshape(vir_count, occ_count * width)
    )
    slots = jnp.arange(batch_size, dtype=jnp.int32)

    def coulomb_term():
        factored = jnp.dot(coulomb_factors, full, preferred_element_type=jnp.float32).astype(
            jnp.bfloat16
        )
        return 2.0 * lax.dot_general(
            coulomb_factors, factored, (((0,), (0,)), ((), ())), preferred_element_type=jnp.float32
        )

    def grid_term(first, last):

        def step(carry, items):
            occ, vir, weight, live = items
            trans = jnp.dot(vir, rearranged, preferred_element_type=jnp.float32).reshape(
                batch_size, occ_count, width
            )
            occ_float = occ.astype(jnp.float32)
            density = jnp.einsum("gik,ig->gk", trans, occ_float)
            mask = (slots < live).astype(jnp.float32)
            weighted = density * (weight * mask)[:, None]
            scaled = (
                (occ_float.T[:, :, None] * weighted[:, None, :])
                .reshape(batch_size, occ_count * width)
                .astype(jnp.bfloat16)
            )
            return (
                carry
                + lax.dot_general(
                    vir, scaled, (((0,), (0,)), ((), ())), preferred_element_type=jnp.float32
                ),
                None,
            )

        start = jnp.zeros((vir_count, occ_count * width), jnp.float32)
        items = (
            occ_values[first:last],
            vir_values[first:last],
            kernel[first:last],
            live_points[first:last],
        )
        total, _ = lax.scan(step, start, items)
        return (
            total.reshape(vir_count, occ_count, width)
            .transpose(1, 0, 2)
            .reshape(occ_count * vir_count, width)
        )

    cut = batches // 2

    def first_group():
        return coulomb_term() + grid_term(0, cut)

    def second_group():
        return grid_term(cut, batches)

    partial_sum = lax.cond(lax.axis_index("grp") == 0, first_group, second_group)
    summed = lax.psum_scatter(partial_sum, ("grp", "blk"), scatter_dimension=0, tiled=True)
    joined = lax.all_to_all(summed, "vec", split_axis=0, concat_axis=1, tiled=True)
    result = energy_gap[:, None] * trial.astype(jnp.float32) + joined
    return result.astype(jnp.bfloat16)


def fused_kernel(
    nz,
    trial_ref,
    gap_ref,
    cf_hbm,
    occ_hbm,
    vir_hbm,
    weight_ref,
    live_ref,
    out_ref,
    full,
    rear,
    cf,
    occ,
    vir,
    scaled,
    exchange,
    partial,
    land_d,
    send_a,
    land_a,
    send_b,
    land_b,
    send_z,
    land_z,
    local_sem,
    load_sem,
    gs_send,
    gs_recv,
    gd_send,
    gd_recv,
    rs_send,
    rs_recv,
    rd_send,
    rd_recv,
):
    f32, bf16 = jnp.float32, jnp.bfloat16
    blocks, _, chunks, width, _ = full.shape
    g, b, v = lax.axis_index("grp"), lax.axis_index("blk"), lax.axis_index("vec")
    z, y = b // 2, lax.rem(b, 2)
    g1, y1 = g + v * (1 - 2 * g), y + (1 - v) * (1 - 2 * y)
    g2, y2 = g + (1 - v) * (1 - 2 * g), y + v * (1 - 2 * y)
    g3, y3 = 1 - g, 1 - y
    quarter = g * 2 + v
    batches, occ_count, part = occ.shape
    vir_count = vir.shape[2]
    cf_rows = cf.shape[0]
    per_occ = vir_count // LANES

    def zed(n):
        return lax.rem(z + nz - n, nz)

    def block(gg, n, yy):
        return gg * (2 * nz) + zed(n) * 2 + yy

    def at(gg, zz, yy, vv):
        return (gg, zz * 2 + yy, vv)

    p1, p2, twin = at(g1, z, y1, v), at(g2, z, y2, v), at(g, z, y, 1 - v)

    barrier = pltpu.get_barrier_semaphore()
    peers = [p1, p2, twin] + [at(g, zed(n), y, v) for n in range(1, nz)]
    for peer in peers:
        pl.semaphore_signal(barrier, inc=1, device_id=peer, device_id_type=MESH)

    own = block(g, 0, y)
    local = [
        pltpu.make_async_copy(
            trial_ref.at[:, pl.ds(c * LANES, LANES)], full.at[own, v, c], local_sem.at[c]
        )
        for c in range(chunks)
    ]
    for copy in local:
        copy.start()
    first_slot = pl.multiple_of(quarter * part, part)
    loads = [
        pltpu.make_async_copy(
            vir_hbm.at[:, pl.ds(first_slot, part), :], vir, load_sem.at[0]
        ),
        pltpu.make_async_copy(
            occ_hbm.at[:, :, pl.ds(first_slot, part)], occ, load_sem.at[1]
        ),
        pltpu.make_async_copy(
            cf_hbm.at[pl.ds(pl.multiple_of(quarter * cf_rows, cf_rows), cf_rows), :],
            cf,
            load_sem.at[2],
        ),
    ]
    for copy in local:
        copy.wait()
    pl.semaphore_wait(barrier, len(peers))

    near = sorted(range(1, nz), key=lambda n: min(n, nz - n))
    sent = []

    def gather(index, sender_block, vv, peer, send, recv):
        return pltpu.make_async_remote_copy(
            src_ref=full.at[sender_block, vv],
            dst_ref=full.at[sender_block, vv],
            send_sem=send.at[index],
            recv_sem=recv.at[index],
            device_id=peer,
            device_id_type=MESH,
        )

    def push(index, blk_index, peer):
        copy = gather(index, blk_index, v, peer, gs_send, gs_recv)
        copy.start()
        sent.append(copy)

    def push_twin(index, blk_index):
        copy = gather(index, blk_index, v, twin, gd_send, gd_recv)
        copy.start()
        sent.append(copy)

    def arrive(index, blk_index):
        gather(index, blk_index, v, p1, gs_send, gs_recv).wait_recv()

    base1, base2 = nz, 2 * nz
    for n in near[::-1]:
        push(n, own, at(g, lax.rem(z + n, nz), y, v))
    push(base1, own, p1)
    push(base2, own, p2)
    push_twin(0, own)
    for copy in loads:
        copy.start()
    for n in near:
        j = block(g, n, y)
        arrive(n, j)
        push(base1 + n, j, p1)
        push(base2 + n, j, p2)
        push_twin(n, j)
    for n in [0] + near:
        j = block(g1, n, y1)
        arrive(base1 + n, j)
        push(base2 + nz + n, j, p2)
        push_twin(nz + n, j)
    for half, (gg, yy) in enumerate(((g2, y2), (g3, y3))):
        for n in [0] + near:
            j = block(gg, n, yy)
            arrive(base2 + half * nz + n, j)
            push_twin((2 + half) * nz + n, j)
    for kind, (gg, yy) in enumerate(((g, y), (g2, y2), (g1, y1), (g3, y3))):
        for n in [0] + near:
            gather(kind * nz + n, block(gg, n, yy), 1 - v, twin, gd_send, gd_recv).wait_recv()
    for copy in sent:
        copy.wait_send()
    for copy in loads:
        copy.wait()

    for i in range(occ_count):
        for c in range(per_occ):
            chunk = i * per_occ + c
            rear[pl.ds(i * width, width), pl.ds(c * LANES, LANES)] = full[
                chunk // (2 * chunks), (chunk // chunks) % 2, chunk % chunks
            ]

    weights = weight_ref[:, pl.ds(first_slot, part)]
    line = lax.broadcasted_iota(jnp.int32, weights.shape, 0)
    slot = first_slot + lax.broadcasted_iota(jnp.int32, (1, part), 1)

    def grid_step(t, _):
        v_t = vir[t]
        trans = lax.dot_general(
            rear[...], v_t, (((1,), (1,)), ((), ())), preferred_element_type=f32
        )
        o = occ[t].astype(f32)
        density = jnp.sum(trans.reshape(occ_count, width, part) * o[:, None, :], axis=0)
        weight = jnp.sum(jnp.where(line == t, weights, 0.0), axis=0, keepdims=True)
        weight = jnp.where(slot < live_ref[t], weight, 0.0)
        weighted = density * weight
        values = (o[:, None, :] * weighted[None, :, :]).reshape(occ_count * width, part)
        scaled[t] = values.astype(bf16)
        return 0

    lax.fori_loop(0, batches, grid_step, 0)

    def factor_step(i, total):
        rows = rear[pl.ds(pl.multiple_of(i * width, width), width), :]
        cols = cf[:, pl.ds(pl.multiple_of(i * vir_count, vir_count), vir_count)]
        return total + lax.dot_general(
            rows, cols, (((1,), (1,)), ((), ())), preferred_element_type=f32
        )

    factored = lax.fori_loop(
        0, occ_count, factor_step, jnp.zeros((width, cf_rows), f32), unroll=4
    )
    doubled = (2.0 * factored.astype(bf16).astype(f32)).astype(bf16)

    group = 5
    rows = (occ_count // group) * width

    def exchange_step(r, _):
        lines = pl.ds(pl.multiple_of(r * rows, rows), rows)
        s = jnp.concatenate([scaled[t, lines, :] for t in range(batches)], axis=1)
        exchange[lines, :] = jnp.dot(
            s, vir[...].reshape(batches * part, vir_count), preferred_element_type=f32
        )
        return 0

    lax.fori_loop(0, group, exchange_step, 0)

    for i in range(occ_count):
        lines = exchange[pl.ds(i * width, width), :] + jnp.dot(
            doubled, cf[:, pl.ds(i * vir_count, vir_count)], preferred_element_type=f32
        )
        for c in range(per_occ):
            chunk = i * per_occ + c
            partial[chunk // (2 * chunks), (chunk // chunks) % 2, chunk % chunks] = lines[
                :, c * LANES : (c + 1) * LANES
            ]

    far = near[::-1] + [0]
    drain = []

    def twin_copy(index, j, vv):
        return pltpu.make_async_remote_copy(
            src_ref=partial.at[j, vv],
            dst_ref=land_d.at[j],
            send_sem=rd_send.at[index],
            recv_sem=rd_recv.at[index],
            device_id=twin,
            device_id_type=MESH,
        )

    for kind, (gg, yy) in enumerate(((g3, y3), (g1, y1), (g2, y2), (g, y))):
        for n in far:
            copy = twin_copy(kind * nz + n, block(gg, n, yy), 1 - v)
            copy.start()
            drain.append(copy)

    def wire(src, dst, slot_index, index, peer):
        return pltpu.make_async_remote_copy(
            src_ref=src.at[slot_index],
            dst_ref=dst.at[slot_index],
            send_sem=rs_send.at[index],
            recv_sem=rs_recv.at[index],
            device_id=peer,
            device_id_type=MESH,
        )

    def pair_sum(kind, n, j):
        twin_copy(kind * nz + n, j, 1 - v).wait_recv()
        return partial[j, v] + land_d[j]

    for kind, (gg, yy) in enumerate(((g3, y3), (g2, y2))):
        for n in far:
            k = kind * nz + n
            send_a[k] = pair_sum(kind, n, block(gg, n, yy)).astype(bf16)
            copy = wire(send_a, land_a, k, k, p2)
            copy.start()
            drain.append(copy)
    for n in far:
        total = pair_sum(2, n, block(g1, n, y1))
        wire(send_a, land_a, n, n, p2).wait_recv()
        send_b[n] = (total + land_a[n].astype(f32)).astype(bf16)
        copy = wire(send_b, land_b, n, 2 * nz + n, p1)
        copy.start()
        drain.append(copy)
    for n in far:
        total = pair_sum(3, n, block(g, n, y))
        wire(send_a, land_a, nz + n, nz + n, p2).wait_recv()
        total = total + land_a[nz + n].astype(f32)
        wire(send_b, land_b, n, 2 * nz + n, p1).wait_recv()
        total = total + land_b[n].astype(f32)
        if n > 0:
            send_z[n - 1] = total.astype(bf16)
            copy = wire(send_z, land_z, n - 1, 3 * nz + n, at(g, zed(n), y, v))
            copy.start()
            drain.append(copy)
    for n in near:
        wire(send_z, land_z, n - 1, 3 * nz + n, p1).wait_recv()
        total = total + land_z[n - 1].astype(f32)
    for c in range(chunks):
        lanes = pl.ds(c * LANES, LANES)
        mine = full[own, v, c].astype(f32)
        out_ref[:, lanes] = (gap_ref[:, lanes] * mine + total[c]).astype(bf16)
    for copy in drain:
        copy.wait_send()


def fused_local(
    blk, trial, energy_gap, coulomb_factors, occ_values, vir_values, kernel, live_points
):
    pairs, width = trial.shape
    blocks = 2 * blk
    nz = blk // 2
    chunks = pairs // LANES
    batches, occ_count, batch_size = occ_values.shape
    vir_count = vir_values.shape[2]
    part = batch_size // 4
    cf_rows = coulomb_factors.shape[0] // 4
    bf16, f32 = jnp.bfloat16, jnp.float32
    vmem = pl.BlockSpec(memory_space=pltpu.VMEM)
    anywhere = pl.BlockSpec(memory_space=pl.ANY)
    dma = pltpu.SemaphoreType.DMA
    out = pl.pallas_call(
        functools.partial(fused_kernel, nz),
        out_shape=jax.ShapeDtypeStruct((width, pairs), bf16),
        in_specs=[
            anywhere,
            vmem,
            anywhere,
            anywhere,
            anywhere,
            vmem,
            pl.BlockSpec(memory_space=pltpu.SMEM),
        ],
        out_specs=vmem,
        scratch_shapes=[
            pltpu.VMEM((blocks, 2, chunks, width, LANES), bf16),
            pltpu.VMEM((occ_count * width, vir_count), bf16),
            pltpu.VMEM((cf_rows, coulomb_factors.shape[1]), bf16),
            pltpu.VMEM((batches, occ_count, part), bf16),
            pltpu.VMEM((batches, part, vir_count), bf16),
            pltpu.VMEM((batches, occ_count * width, part), bf16),
            pltpu.VMEM((occ_count * width, vir_count), f32),
            pltpu.VMEM((blocks, 2, chunks, width, LANES), f32),
            pltpu.VMEM((blocks, chunks, width, LANES), f32),
            pltpu.VMEM((2 * nz, chunks, width, LANES), bf16),
            pltpu.VMEM((2 * nz, chunks, width, LANES), bf16),
            pltpu.VMEM((nz, chunks, width, LANES), bf16),
            pltpu.VMEM((nz, chunks, width, LANES), bf16),
            pltpu.VMEM((nz, chunks, width, LANES), bf16),
            pltpu.VMEM((nz, chunks, width, LANES), bf16),
            dma((chunks,)),
            dma((3,)),
            dma((4 * nz,)),
            dma((4 * nz,)),
            dma((4 * nz,)),
            dma((4 * nz,)),
            dma((4 * nz,)),
            dma((4 * nz,)),
            dma((4 * nz,)),
            dma((4 * nz,)),
        ],
        compiler_params=pltpu.CompilerParams(
            collective_id=0, has_side_effects=True, vmem_limit_bytes=56 * 1024 * 1024
        ),
    )(
        trial.T,
        energy_gap[None, :],
        coulomb_factors,
        occ_values,
        vir_values,
        kernel,
        live_points,
    )
    return out.T


def fits(mesh):
    def check(trial, coulomb_factors, occ_values, vir_values):
        return (
            mesh.shape["grp"] == 2
            and mesh.shape["vec"] == 2
            and mesh.shape["blk"] % 4 == 0
            and trial.shape[0] % LANES == 0
            and coulomb_factors.shape[0] % (4 * LANES) == 0
            and occ_values.shape[2] % (4 * LANES) == 0
            and occ_values.shape[1] % 5 == 0
            and vir_values.shape[2] % LANES == 0
        )

    return check


def solution(mesh):
    in_specs = (
        P(("grp", "blk", "vec"), None),
        P(("grp", "blk", "vec")),
        P("blk", None),
        P("blk", None, None),
        P("blk", None, None),
        P("blk", None),
        P("blk"),
    )
    out_specs = P(("grp", "blk", "vec"), None)
    check = fits(mesh)

    def local(trial, energy_gap, coulomb_factors, occ_values, vir_values, kernel, live_points):
        args = (trial, energy_gap, coulomb_factors, occ_values, vir_values, kernel, live_points)
        if check(trial, coulomb_factors, occ_values, vir_values):
            return fused_local(mesh.shape["blk"], *args)
        return collective_local(*args)

    return jax.shard_map(local, mesh=mesh, in_specs=in_specs, out_specs=out_specs, check_vma=False)
```

```python
import functools

import jax
import jax.numpy as jnp
from jax import lax
from jax.experimental import pallas as pl
from jax.experimental.pallas import tpu as pltpu
from jax.sharding import PartitionSpec as P

LANES = 128
MESH = pl.DeviceIdType.MESH


def collective_local(
    trial, energy_gap, coulomb_factors, occ_values, vir_values, kernel, live_points
):
    pair_rows = lax.all_to_all(trial, "vec", split_axis=1, concat_axis=0, tiled=True)
    full = lax.all_gather(pair_rows, ("grp", "blk"), axis=0, tiled=True)
    occ_count = occ_values.shape[1]
    batch_size = occ_values.shape[2]
    vir_count = vir_values.shape[2]
    width = full.shape[1]
    batches = occ_values.shape[0]
    rearranged = (
        full.reshape(occ_count, vir_count, width)
        .transpose(1, 0, 2)
        .reshape(vir_count, occ_count * width)
    )
    slots = jnp.arange(batch_size, dtype=jnp.int32)

    def coulomb_term():
        factored = jnp.dot(coulomb_factors, full, preferred_element_type=jnp.float32).astype(
            jnp.bfloat16
        )
        return 2.0 * lax.dot_general(
            coulomb_factors, factored, (((0,), (0,)), ((), ())), preferred_element_type=jnp.float32
        )

    def grid_term(first, last):

        def step(carry, items):
            occ, vir, weight, live = items
            trans = jnp.dot(vir, rearranged, preferred_element_type=jnp.float32).reshape(
                batch_size, occ_count, width
            )
            occ_float = occ.astype(jnp.float32)
            density = jnp.einsum("gik,ig->gk", trans, occ_float)
            mask = (slots < live).astype(jnp.float32)
            weighted = density * (weight * mask)[:, None]
            scaled = (
                (occ_float.T[:, :, None] * weighted[:, None, :])
                .reshape(batch_size, occ_count * width)
                .astype(jnp.bfloat16)
            )
            return (
                carry
                + lax.dot_general(
                    vir, scaled, (((0,), (0,)), ((), ())), preferred_element_type=jnp.float32
                ),
                None,
            )

        start = jnp.zeros((vir_count, occ_count * width), jnp.float32)
        items = (
            occ_values[first:last],
            vir_values[first:last],
            kernel[first:last],
            live_points[first:last],
        )
        total, _ = lax.scan(step, start, items)
        return (
            total.reshape(vir_count, occ_count, width)
            .transpose(1, 0, 2)
            .reshape(occ_count * vir_count, width)
        )

    cut = batches // 2

    def first_group():
        return coulomb_term() + grid_term(0, cut)

    def second_group():
        return grid_term(cut, batches)

    partial_sum = lax.cond(lax.axis_index("grp") == 0, first_group, second_group)
    summed = lax.psum_scatter(partial_sum, ("grp", "blk"), scatter_dimension=0, tiled=True)
    joined = lax.all_to_all(summed, "vec", split_axis=0, concat_axis=1, tiled=True)
    result = energy_gap[:, None] * trial.astype(jnp.float32) + joined
    return result.astype(jnp.bfloat16)


def fused_kernel(
    nz,
    trial_ref,
    cf_hbm,
    occ_hbm,
    vir_hbm,
    weight_ref,
    live_ref,
    out_ref,
    full,
    rear,
    cf,
    occ,
    occ_float,
    vir,
    density,
    factored,
    partial,
    land_d,
    send_a,
    land_a,
    send_b,
    land_b,
    send_z,
    land_z,
    local_sem,
    load_sem,
    gs_send,
    gs_recv,
    gd_send,
    gd_recv,
    rs_send,
    rs_recv,
    rd_send,
    rd_recv,
):
    f32, bf16 = jnp.float32, jnp.bfloat16
    _, _, chunks, width, _ = full.shape
    g, b, v = lax.axis_index("grp"), lax.axis_index("blk"), lax.axis_index("vec")
    z, y = b // 2, lax.rem(b, 2)
    g1, y1 = g + v * (1 - 2 * g), y + (1 - v) * (1 - 2 * y)
    g2, y2 = g + (1 - v) * (1 - 2 * g), y + v * (1 - 2 * y)
    g3, y3 = 1 - g, 1 - y
    kind1, kind2 = 1 + v, 2 - v
    quarter = g * 2 + v
    batches, occ_count, part = occ.shape
    vir_count = vir.shape[2]
    points = batches * part
    cf_rows = cf.shape[0]
    per_occ = vir_count // LANES
    group_occ = 4 * chunks // per_occ
    lines = group_occ * width
    step = 2 if batches % 2 == 0 else 1

    def zed(n):
        return lax.rem(z + nz - n, nz)

    def block(gg, n, yy):
        return gg * (2 * nz) + zed(n) * 2 + yy

    def at(gg, zz, yy, vv):
        return (gg, zz * 2 + yy, vv)

    p1, p2, twin = at(g1, z, y1, v), at(g2, z, y2, v), at(g, z, y, 1 - v)

    barrier = pltpu.get_barrier_semaphore()
    peers = [p1, p2, twin] + [at(g, zed(n), y, v) for n in range(1, nz)]
    for peer in peers:
        pl.semaphore_signal(barrier, inc=1, device_id=peer, device_id_type=MESH)

    own = block(g, 0, y)
    local = [
        pltpu.make_async_copy(
            trial_ref.at[:, pl.ds(c * LANES, LANES)], full.at[own, v, c], local_sem.at[c]
        )
        for c in range(chunks)
    ]
    for copy in local:
        copy.start()
    first_slot = pl.multiple_of(quarter * part, part)
    loads = [
        pltpu.make_async_copy(
            occ_hbm.at[:, :, pl.ds(first_slot, part)], occ, load_sem.at[0]
        ),
        pltpu.make_async_copy(
            vir_hbm.at[:, pl.ds(first_slot, part), :], vir, load_sem.at[1]
        ),
        pltpu.make_async_copy(
            cf_hbm.at[pl.ds(pl.multiple_of(quarter * cf_rows, cf_rows), cf_rows), :],
            cf,
            load_sem.at[2],
        ),
    ]
    for copy in loads:
        copy.start()
    for copy in local:
        copy.wait()
    pl.semaphore_wait(barrier, len(peers))

    near = sorted(range(1, nz), key=lambda n: min(n, nz - n))
    order = [0] + near
    sent = []

    def gather(index, j, vv, peer, send, recv):
        return pltpu.make_async_remote_copy(
            src_ref=full.at[j, vv],
            dst_ref=full.at[j, vv],
            send_sem=send.at[index],
            recv_sem=recv.at[index],
            device_id=peer,
            device_id_type=MESH,
        )

    def push(index, j, peer):
        copy = gather(index, j, v, peer, gs_send, gs_recv)
        copy.start()
        sent.append(copy)

    def push_twin(kind, n, j):
        copy = gather(kind * nz + n, j, v, twin, gd_send, gd_recv)
        copy.start()
        sent.append(copy)

    def arrive(index, j):
        gather(index, j, v, p1, gs_send, gs_recv).wait_recv()

    def from_twin(kind, n, j):
        gather(kind * nz + n, j, 1 - v, twin, gd_send, gd_recv).wait_recv()

    def absorb(gg, fx, n, slot):
        from_twin(2 * fx, n, block(gg, n, y))
        from_twin(2 * fx + 1, n, block(gg, n, y3))
        group = gg * nz + zed(n)
        for m in range(4 * chunks):
            i, c = m // per_occ, m % per_occ
            rear[slot, i * width : (i + 1) * width, c * LANES : (c + 1) * LANES] = full[
                group * 2 + m // (2 * chunks), (m // chunks) % 2, m % chunks
            ]
        for t in range(0, batches, step):
            span = slice(t * part, (t + step) * part)
            trans = lax.dot_general(
                rear[slot],
                vir[t : t + step].reshape(step * part, vir_count),
                (((1,), (1,)), ((), ())),
                preferred_element_type=f32,
            )
            o = occ_float[group, :, span]
            term = jnp.sum(trans.reshape(group_occ, width, step * part) * o[:, None, :], axis=0)
            density[:, span] = term if slot == 0 else density[:, span] + term
        total = None
        for i in range(group_occ):
            start = pl.multiple_of((group * group_occ + i) * vir_count, vir_count)
            term = lax.dot_general(
                rear[slot, i * width : (i + 1) * width, :],
                cf[:, pl.ds(start, vir_count)],
                (((1,), (1,)), ((), ())),
                preferred_element_type=f32,
            )
            total = term if total is None else total + term
        factored[...] = total if slot == 0 else factored[...] + total

    base1, base2 = nz, 2 * nz
    for n in near[::-1]:
        push(n, own, at(g, lax.rem(z + n, nz), y, v))
    push(base1, own, p1)
    push(base2, own, p2)
    push_twin(0, 0, own)
    loads[0].wait()
    for k in range(2 * nz):
        for t in range(batches):
            occ_float[k, :, t * part : (t + 1) * part] = occ[
                t, k * group_occ : (k + 1) * group_occ, :
            ].astype(f32)

    def second(n):
        j = block(g1, n, y1)
        arrive(base1 + n, j)
        push(base2 + nz + n, j, p2)
        push_twin(kind1, n, j)
        j = block(g2, n, y2)
        arrive(base2 + n, j)
        push_twin(kind2, n, j)

    second(0)
    for n in near:
        j = block(g, n, y)
        arrive(n, j)
        push(base1 + n, j, p1)
        push(base2 + n, j, p2)
        push_twin(0, n, j)
    loads[1].wait()
    loads[2].wait()
    for k, n in enumerate(order):
        if k > 0:
            second(n)
            absorb(g, 0, order[k - 1], k - 1)
    for k, n in enumerate(order):
        j = block(g3, n, y3)
        arrive(base2 + nz + n, j)
        push_twin(3, n, j)
        if k == 0:
            absorb(g, 0, order[-1], nz - 1)
        else:
            absorb(g3, 1, order[k - 1], nz + k - 1)
    absorb(g3, 1, order[-1], 2 * nz - 1)

    weights = weight_ref[:, pl.ds(first_slot, part)]
    place = first_slot + lax.broadcasted_iota(jnp.int32, (1, part), 1)
    for t in range(batches):
        span = slice(t * part, (t + 1) * part)
        weight = jnp.where(place < live_ref[t], weights[t : t + 1, :], 0.0)
        density[:, span] = density[:, span] * weight
    doubled = (2.0 * factored[...].astype(bf16).astype(f32)).astype(bf16)

    def terms(gg, n):
        group = gg * nz + zed(n)
        pieces = []
        for t in range(batches):
            span = slice(t * part, (t + 1) * part)
            o = occ_float[group, :, span]
            pieces.append(
                (o[:, None, :] * density[:, span][None, :, :]).reshape(lines, part).astype(bf16)
            )
        exchange = jnp.dot(
            jnp.concatenate(pieces, axis=1),
            vir[...].reshape(points, vir_count),
            preferred_element_type=f32,
        )
        for i in range(group_occ):
            start = pl.multiple_of((group * group_occ + i) * vir_count, vir_count)
            both = exchange[i * width : (i + 1) * width, :] + jnp.dot(
                doubled, cf[:, pl.ds(start, vir_count)], preferred_element_type=f32
            )
            for c in range(per_occ):
                m = i * per_occ + c
                partial[group * 2 + m // (2 * chunks), (m // chunks) % 2, m % chunks] = both[
                    :, c * LANES : (c + 1) * LANES
                ]

    far = near[::-1] + [0]
    drain = []

    def twin_copy(kind, n, j, vv):
        return pltpu.make_async_remote_copy(
            src_ref=partial.at[j, vv],
            dst_ref=land_d.at[j],
            send_sem=rd_send.at[kind * nz + n],
            recv_sem=rd_recv.at[kind * nz + n],
            device_id=twin,
            device_id_type=MESH,
        )

    def wire(src, dst, slot, index, peer):
        return pltpu.make_async_remote_copy(
            src_ref=src.at[slot],
            dst_ref=dst.at[slot],
            send_sem=rs_send.at[index],
            recv_sem=rs_recv.at[index],
            device_id=peer,
            device_id_type=MESH,
        )

    def pair_sum(kind, n, j):
        twin_copy(kind, n, j, 1 - v).wait_recv()
        return partial[j, v] + land_d[j]

    def give(copy):
        copy.start()
        drain.append(copy)

    def stage_a(n):
        for half, (kind, gg, yy) in enumerate(((3, g3, y3), (kind2, g2, y2))):
            k = half * nz + n
            send_a[k] = pair_sum(kind, n, block(gg, n, yy)).astype(bf16)
            give(wire(send_a, land_a, k, k, p2))

    for k, n in enumerate(far):
        for fx, gg in ((1, g3), (0, g)):
            terms(gg, n)
            for fy, yy in ((1, y3), (0, y)):
                give(twin_copy(2 * fx + fy, n, block(gg, n, yy), 1 - v))
            if fx == 1 and k > 0:
                stage_a(far[k - 1])
    stage_a(far[-1])
    for n in far:
        total = pair_sum(kind1, n, block(g1, n, y1))
        wire(send_a, land_a, n, n, p2).wait_recv()
        send_b[n] = (total + land_a[n].astype(f32)).astype(bf16)
        give(wire(send_b, land_b, n, 2 * nz + n, p1))
    for n in far:
        total = pair_sum(0, n, block(g, n, y))
        wire(send_a, land_a, nz + n, nz + n, p2).wait_recv()
        total = total + land_a[nz + n].astype(f32)
        wire(send_b, land_b, n, 2 * nz + n, p1).wait_recv()
        total = total + land_b[n].astype(f32)
        if n > 0:
            send_z[n - 1] = total.astype(bf16)
            give(wire(send_z, land_z, n - 1, 3 * nz + n, at(g, zed(n), y, v)))
    for n in near:
        wire(send_z, land_z, n - 1, 3 * nz + n, p1).wait_recv()
        total = total + land_z[n - 1].astype(f32)
    for c in range(chunks):
        out_ref[:, c * LANES : (c + 1) * LANES] = total[c]
    for copy in sent + drain:
        copy.wait_send()


def fused_local(
    blk, trial, energy_gap, coulomb_factors, occ_values, vir_values, kernel, live_points
):
    pairs, width = trial.shape
    blocks = 2 * blk
    nz = blk // 2
    chunks = pairs // LANES
    batches, occ_count, batch_size = occ_values.shape
    vir_count = vir_values.shape[2]
    part = batch_size // 4
    cf_rows = coulomb_factors.shape[0] // 4
    group_occ = occ_count // blk
    bf16, f32 = jnp.bfloat16, jnp.float32
    vmem = pl.BlockSpec(memory_space=pltpu.VMEM)
    anywhere = pl.BlockSpec(memory_space=pl.ANY)
    dma = pltpu.SemaphoreType.DMA
    total = pl.pallas_call(
        functools.partial(fused_kernel, nz),
        out_shape=jax.ShapeDtypeStruct((width, pairs), f32),
        in_specs=[
            anywhere,
            anywhere,
            anywhere,
            anywhere,
            vmem,
            pl.BlockSpec(memory_space=pltpu.SMEM),
        ],
        out_specs=vmem,
        scratch_shapes=[
            pltpu.VMEM((blocks, 2, chunks, width, LANES), bf16),
            pltpu.VMEM((2 * nz, group_occ * width, vir_count), bf16),
            pltpu.VMEM((cf_rows, coulomb_factors.shape[1]), bf16),
            pltpu.VMEM((batches, occ_count, part), bf16),
            pltpu.VMEM((2 * nz, group_occ, batches * part), f32),
            pltpu.VMEM((batches, part, vir_count), bf16),
            pltpu.VMEM((width, batches * part), f32),
            pltpu.VMEM((width, cf_rows), f32),
            pltpu.VMEM((blocks, 2, chunks, width, LANES), f32),
            pltpu.VMEM((blocks, chunks, width, LANES), f32),
            pltpu.VMEM((2 * nz, chunks, width, LANES), bf16),
            pltpu.VMEM((2 * nz, chunks, width, LANES), bf16),
            pltpu.VMEM((nz, chunks, width, LANES), bf16),
            pltpu.VMEM((nz, chunks, width, LANES), bf16),
            pltpu.VMEM((nz, chunks, width, LANES), bf16),
            pltpu.VMEM((nz, chunks, width, LANES), bf16),
            dma((chunks,)),
            dma((3,)),
            dma((4 * nz,)),
            dma((4 * nz,)),
            dma((4 * nz,)),
            dma((4 * nz,)),
            dma((4 * nz,)),
            dma((4 * nz,)),
            dma((4 * nz,)),
            dma((4 * nz,)),
        ],
        compiler_params=pltpu.CompilerParams(
            collective_id=0, has_side_effects=True, vmem_limit_bytes=56 * 1024 * 1024
        ),
    )(trial.T, coulomb_factors, occ_values, vir_values, kernel, live_points)
    result = energy_gap[:, None] * trial.astype(f32) + total.T
    return result.astype(bf16)


def fits(mesh):
    def check(trial, coulomb_factors, occ_values, vir_values):
        return (
            mesh.shape["grp"] == 2
            and mesh.shape["vec"] == 2
            and mesh.shape["blk"] % 4 == 0
            and trial.shape[0] % LANES == 0
            and coulomb_factors.shape[0] % (4 * LANES) == 0
            and occ_values.shape[2] % (4 * LANES) == 0
            and occ_values.shape[1] % mesh.shape["blk"] == 0
            and vir_values.shape[2] % LANES == 0
        )

    return check


def solution(mesh):
    in_specs = (
        P(("grp", "blk", "vec"), None),
        P(("grp", "blk", "vec")),
        P("blk", None),
        P("blk", None, None),
        P("blk", None, None),
        P("blk", None),
        P("blk"),
    )
    out_specs = P(("grp", "blk", "vec"), None)
    check = fits(mesh)

    def local(trial, energy_gap, coulomb_factors, occ_values, vir_values, kernel, live_points):
        args = (trial, energy_gap, coulomb_factors, occ_values, vir_values, kernel, live_points)
        if check(trial, coulomb_factors, occ_values, vir_values):
            return fused_local(mesh.shape["blk"], *args)
        return collective_local(*args)

    return jax.shard_map(local, mesh=mesh, in_specs=in_specs, out_specs=out_specs, check_vma=False)
```

```python
import functools

import jax
import jax.numpy as jnp
from jax import lax
from jax.experimental import pallas as pl
from jax.experimental.pallas import tpu as pltpu
from jax.sharding import PartitionSpec as P

LANES = 128
MESH = pl.DeviceIdType.MESH


def collective_local(
    trial, energy_gap, coulomb_factors, occ_values, vir_values, kernel, live_points
):
    pair_rows = lax.all_to_all(trial, "vec", split_axis=1, concat_axis=0, tiled=True)
    full = lax.all_gather(pair_rows, ("grp", "blk"), axis=0, tiled=True)
    occ_count = occ_values.shape[1]
    batch_size = occ_values.shape[2]
    vir_count = vir_values.shape[2]
    width = full.shape[1]
    batches = occ_values.shape[0]
    rearranged = (
        full.reshape(occ_count, vir_count, width)
        .transpose(1, 0, 2)
        .reshape(vir_count, occ_count * width)
    )
    slots = jnp.arange(batch_size, dtype=jnp.int32)

    def coulomb_term():
        factored = jnp.dot(coulomb_factors, full, preferred_element_type=jnp.float32).astype(
            jnp.bfloat16
        )
        return 2.0 * lax.dot_general(
            coulomb_factors, factored, (((0,), (0,)), ((), ())), preferred_element_type=jnp.float32
        )

    def grid_term(first, last):

        def step(carry, items):
            occ, vir, weight, live = items
            trans = jnp.dot(vir, rearranged, preferred_element_type=jnp.float32).reshape(
                batch_size, occ_count, width
            )
            occ_float = occ.astype(jnp.float32)
            density = jnp.einsum("gik,ig->gk", trans, occ_float)
            mask = (slots < live).astype(jnp.float32)
            weighted = density * (weight * mask)[:, None]
            scaled = (
                (occ_float.T[:, :, None] * weighted[:, None, :])
                .reshape(batch_size, occ_count * width)
                .astype(jnp.bfloat16)
            )
            return (
                carry
                + lax.dot_general(
                    vir, scaled, (((0,), (0,)), ((), ())), preferred_element_type=jnp.float32
                ),
                None,
            )

        start = jnp.zeros((vir_count, occ_count * width), jnp.float32)
        items = (
            occ_values[first:last],
            vir_values[first:last],
            kernel[first:last],
            live_points[first:last],
        )
        total, _ = lax.scan(step, start, items)
        return (
            total.reshape(vir_count, occ_count, width)
            .transpose(1, 0, 2)
            .reshape(occ_count * vir_count, width)
        )

    cut = batches // 2

    def first_group():
        return coulomb_term() + grid_term(0, cut)

    def second_group():
        return grid_term(cut, batches)

    partial_sum = lax.cond(lax.axis_index("grp") == 0, first_group, second_group)
    summed = lax.psum_scatter(partial_sum, ("grp", "blk"), scatter_dimension=0, tiled=True)
    joined = lax.all_to_all(summed, "vec", split_axis=0, concat_axis=1, tiled=True)
    result = energy_gap[:, None] * trial.astype(jnp.float32) + joined
    return result.astype(jnp.bfloat16)


def fused_kernel(
    nz,
    trial_ref,
    cf_hbm,
    occ_hbm,
    vir_hbm,
    weight_ref,
    live_ref,
    out_ref,
    full,
    rear,
    cf,
    occ,
    occ_float,
    vir,
    density,
    factored,
    partial,
    land_d,
    send_a,
    land_a,
    send_b,
    land_b,
    send_z,
    land_z,
    local_sem,
    load_sem,
    gs_send,
    gs_recv,
    gd_send,
    gd_recv,
    rs_send,
    rs_recv,
    rd_send,
    rd_recv,
):
    f32, bf16 = jnp.float32, jnp.bfloat16
    _, _, chunks, width, _ = full.shape
    g, b, v = lax.axis_index("grp"), lax.axis_index("blk"), lax.axis_index("vec")
    z, y = b // 2, lax.rem(b, 2)
    g1, y1 = g + v * (1 - 2 * g), y + (1 - v) * (1 - 2 * y)
    g2, y2 = g + (1 - v) * (1 - 2 * g), y + v * (1 - 2 * y)
    g3, y3 = 1 - g, 1 - y
    kind1, kind2 = 1 + v, 2 - v
    quarter = g * 2 + v
    batches, occ_count, part = occ.shape
    vir_count = vir.shape[2]
    points = batches * part
    cf_rows = cf.shape[0]
    per_occ = vir_count // LANES
    group_occ = 4 * chunks // per_occ
    lines = group_occ * width
    step = 2 if batches % 2 == 0 else 1

    def zed(n):
        other = z
        for k in range(nz.bit_length() - 1):
            if n >> k & 1:
                other = other + (1 - 2 * lax.rem(z // 2**k, 2)) * 2**k
        return other

    def block(gg, n, yy):
        return gg * (2 * nz) + zed(n) * 2 + yy

    def at(gg, zz, yy, vv):
        return (gg, zz * 2 + yy, vv)

    p1, p2, twin = at(g1, z, y1, v), at(g2, z, y2, v), at(g, z, y, 1 - v)

    barrier = pltpu.get_barrier_semaphore()
    peers = [p1, p2, twin] + [at(g, zed(n), y, v) for n in range(1, nz)]
    for peer in peers:
        pl.semaphore_signal(barrier, inc=1, device_id=peer, device_id_type=MESH)

    own = block(g, 0, y)
    local = [
        pltpu.make_async_copy(
            trial_ref.at[:, pl.ds(c * LANES, LANES)], full.at[own, v, c], local_sem.at[c]
        )
        for c in range(chunks)
    ]
    for copy in local:
        copy.start()
    first_slot = pl.multiple_of(quarter * part, part)
    loads = [
        pltpu.make_async_copy(
            occ_hbm.at[:, :, pl.ds(first_slot, part)], occ, load_sem.at[0]
        ),
        pltpu.make_async_copy(
            vir_hbm.at[:, pl.ds(first_slot, part), :], vir, load_sem.at[1]
        ),
        pltpu.make_async_copy(
            cf_hbm.at[pl.ds(pl.multiple_of(quarter * cf_rows, cf_rows), cf_rows), :],
            cf,
            load_sem.at[2],
        ),
    ]
    for copy in loads:
        copy.start()
    for copy in local:
        copy.wait()
    pl.semaphore_wait(barrier, len(peers))

    near = list(range(1, nz))
    order = [0] + near
    sent = []

    def gather(index, j, vv, peer, send, recv):
        return pltpu.make_async_remote_copy(
            src_ref=full.at[j, vv],
            dst_ref=full.at[j, vv],
            send_sem=send.at[index],
            recv_sem=recv.at[index],
            device_id=peer,
            device_id_type=MESH,
        )

    def push(index, j, peer):
        copy = gather(index, j, v, peer, gs_send, gs_recv)
        copy.start()
        sent.append(copy)

    def push_twin(kind, n, j):
        copy = gather(kind * nz + n, j, v, twin, gd_send, gd_recv)
        copy.start()
        sent.append(copy)

    def arrive(index, j):
        gather(index, j, v, p1, gs_send, gs_recv).wait_recv()

    def from_twin(kind, n, j):
        gather(kind * nz + n, j, 1 - v, twin, gd_send, gd_recv).wait_recv()

    def absorb(gg, fx, n, slot):
        from_twin(2 * fx, n, block(gg, n, y))
        from_twin(2 * fx + 1, n, block(gg, n, y3))
        group = gg * nz + zed(n)
        for m in range(4 * chunks):
            i, c = m // per_occ, m % per_occ
            rear[slot, i * width : (i + 1) * width, c * LANES : (c + 1) * LANES] = full[
                group * 2 + m // (2 * chunks), (m // chunks) % 2, m % chunks
            ]
        for t in range(0, batches, step):
            span = slice(t * part, (t + step) * part)
            trans = lax.dot_general(
                rear[slot],
                vir[t : t + step].reshape(step * part, vir_count),
                (((1,), (1,)), ((), ())),
                preferred_element_type=f32,
            )
            o = occ_float[group, :, span]
            term = jnp.sum(trans.reshape(group_occ, width, step * part) * o[:, None, :], axis=0)
            density[:, span] = term if slot == 0 else density[:, span] + term
        total = None
        for i in range(group_occ):
            start = pl.multiple_of((group * group_occ + i) * vir_count, vir_count)
            term = lax.dot_general(
                rear[slot, i * width : (i + 1) * width, :],
                cf[:, pl.ds(start, vir_count)],
                (((1,), (1,)), ((), ())),
                preferred_element_type=f32,
            )
            total = term if total is None else total + term
        factored[...] = total if slot == 0 else factored[...] + total

    base1, base2 = nz, 2 * nz
    for n in near:
        push(n, own, at(g, zed(n), y, v))
    push(base1, own, p1)
    push(base2, own, p2)
    push_twin(0, 0, own)
    loads[0].wait()
    for k in range(2 * nz):
        for t in range(batches):
            occ_float[k, :, t * part : (t + 1) * part] = occ[
                t, k * group_occ : (k + 1) * group_occ, :
            ].astype(f32)

    def second(n):
        j = block(g1, n, y1)
        arrive(base1 + n, j)
        push(base2 + nz + n, j, p2)
        push_twin(kind1, n, j)
        j = block(g2, n, y2)
        arrive(base2 + n, j)
        push_twin(kind2, n, j)

    second(0)
    for n in near:
        j = block(g, n, y)
        arrive(n, j)
        push(base1 + n, j, p1)
        push(base2 + n, j, p2)
        push_twin(0, n, j)
    loads[1].wait()
    loads[2].wait()
    for k, n in enumerate(order):
        if k > 0:
            second(n)
            absorb(g, 0, order[k - 1], k - 1)
    for k, n in enumerate(order):
        j = block(g3, n, y3)
        arrive(base2 + nz + n, j)
        push_twin(3, n, j)
        if k == 0:
            absorb(g, 0, order[-1], nz - 1)
        else:
            absorb(g3, 1, order[k - 1], nz + k - 1)
    absorb(g3, 1, order[-1], 2 * nz - 1)

    weights = weight_ref[:, pl.ds(first_slot, part)]
    place = first_slot + lax.broadcasted_iota(jnp.int32, (1, part), 1)
    for t in range(batches):
        span = slice(t * part, (t + 1) * part)
        weight = jnp.where(place < live_ref[t], weights[t : t + 1, :], 0.0)
        density[:, span] = density[:, span] * weight
    doubled = (2.0 * factored[...].astype(bf16).astype(f32)).astype(bf16)

    def terms(gg, n):
        group = gg * nz + zed(n)
        pieces = []
        for t in range(batches):
            span = slice(t * part, (t + 1) * part)
            o = occ_float[group, :, span]
            pieces.append(
                (o[:, None, :] * density[:, span][None, :, :]).reshape(lines, part).astype(bf16)
            )
        exchange = jnp.dot(
            jnp.concatenate(pieces, axis=1),
            vir[...].reshape(points, vir_count),
            preferred_element_type=f32,
        )
        for i in range(group_occ):
            start = pl.multiple_of((group * group_occ + i) * vir_count, vir_count)
            both = exchange[i * width : (i + 1) * width, :] + jnp.dot(
                doubled, cf[:, pl.ds(start, vir_count)], preferred_element_type=f32
            )
            for c in range(per_occ):
                m = i * per_occ + c
                partial[group * 2 + m // (2 * chunks), (m // chunks) % 2, m % chunks] = both[
                    :, c * LANES : (c + 1) * LANES
                ]

    last_own = near + [0]
    drain = []

    def twin_copy(kind, n, j, vv):
        return pltpu.make_async_remote_copy(
            src_ref=partial.at[j, vv],
            dst_ref=land_d.at[j],
            send_sem=rd_send.at[kind * nz + n],
            recv_sem=rd_recv.at[kind * nz + n],
            device_id=twin,
            device_id_type=MESH,
        )

    def wire(src, dst, slot, index, peer):
        return pltpu.make_async_remote_copy(
            src_ref=src.at[slot],
            dst_ref=dst.at[slot],
            send_sem=rs_send.at[index],
            recv_sem=rs_recv.at[index],
            device_id=peer,
            device_id_type=MESH,
        )

    def pair_sum(kind, n, j):
        twin_copy(kind, n, j, 1 - v).wait_recv()
        return partial[j, v] + land_d[j]

    def give(copy):
        copy.start()
        drain.append(copy)

    def stage_a(n):
        for half, (kind, gg, yy) in enumerate(((3, g3, y3), (kind2, g2, y2))):
            k = half * nz + n
            send_a[k] = pair_sum(kind, n, block(gg, n, yy)).astype(bf16)
            give(wire(send_a, land_a, k, k, p2))

    for k, n in enumerate(last_own):
        for fx, gg in ((1, g3), (0, g)):
            terms(gg, n)
            for fy, yy in ((1, y3), (0, y)):
                give(twin_copy(2 * fx + fy, n, block(gg, n, yy), 1 - v))
            if fx == 1 and k > 0:
                stage_a(last_own[k - 1])
    stage_a(last_own[-1])
    for n in last_own:
        total = pair_sum(kind1, n, block(g1, n, y1))
        wire(send_a, land_a, n, n, p2).wait_recv()
        send_b[n] = (total + land_a[n].astype(f32)).astype(bf16)
        give(wire(send_b, land_b, n, 2 * nz + n, p1))
    for n in last_own:
        total = pair_sum(0, n, block(g, n, y))
        wire(send_a, land_a, nz + n, nz + n, p2).wait_recv()
        total = total + land_a[nz + n].astype(f32)
        wire(send_b, land_b, n, 2 * nz + n, p1).wait_recv()
        total = total + land_b[n].astype(f32)
        if n > 0:
            send_z[n - 1] = total.astype(bf16)
            give(wire(send_z, land_z, n - 1, 3 * nz + n, at(g, zed(n), y, v)))
    for n in near:
        wire(send_z, land_z, n - 1, 3 * nz + n, p1).wait_recv()
        total = total + land_z[n - 1].astype(f32)
    for c in range(chunks):
        out_ref[:, c * LANES : (c + 1) * LANES] = total[c]
    for copy in sent + drain:
        copy.wait_send()


def fused_local(
    blk, trial, energy_gap, coulomb_factors, occ_values, vir_values, kernel, live_points
):
    pairs, width = trial.shape
    blocks = 2 * blk
    nz = blk // 2
    chunks = pairs // LANES
    batches, occ_count, batch_size = occ_values.shape
    vir_count = vir_values.shape[2]
    part = batch_size // 4
    cf_rows = coulomb_factors.shape[0] // 4
    group_occ = occ_count // blk
    bf16, f32 = jnp.bfloat16, jnp.float32
    vmem = pl.BlockSpec(memory_space=pltpu.VMEM)
    anywhere = pl.BlockSpec(memory_space=pl.ANY)
    dma = pltpu.SemaphoreType.DMA
    total = pl.pallas_call(
        functools.partial(fused_kernel, nz),
        out_shape=jax.ShapeDtypeStruct((width, pairs), f32),
        in_specs=[
            anywhere,
            anywhere,
            anywhere,
            anywhere,
            vmem,
            pl.BlockSpec(memory_space=pltpu.SMEM),
        ],
        out_specs=vmem,
        scratch_shapes=[
            pltpu.VMEM((blocks, 2, chunks, width, LANES), bf16),
            pltpu.VMEM((2 * nz, group_occ * width, vir_count), bf16),
            pltpu.VMEM((cf_rows, coulomb_factors.shape[1]), bf16),
            pltpu.VMEM((batches, occ_count, part), bf16),
            pltpu.VMEM((2 * nz, group_occ, batches * part), f32),
            pltpu.VMEM((batches, part, vir_count), bf16),
            pltpu.VMEM((width, batches * part), f32),
            pltpu.VMEM((width, cf_rows), f32),
            pltpu.VMEM((blocks, 2, chunks, width, LANES), f32),
            pltpu.VMEM((blocks, chunks, width, LANES), f32),
            pltpu.VMEM((2 * nz, chunks, width, LANES), bf16),
            pltpu.VMEM((2 * nz, chunks, width, LANES), bf16),
            pltpu.VMEM((nz, chunks, width, LANES), bf16),
            pltpu.VMEM((nz, chunks, width, LANES), bf16),
            pltpu.VMEM((nz, chunks, width, LANES), bf16),
            pltpu.VMEM((nz, chunks, width, LANES), bf16),
            dma((chunks,)),
            dma((3,)),
            dma((4 * nz,)),
            dma((4 * nz,)),
            dma((4 * nz,)),
            dma((4 * nz,)),
            dma((4 * nz,)),
            dma((4 * nz,)),
            dma((4 * nz,)),
            dma((4 * nz,)),
        ],
        compiler_params=pltpu.CompilerParams(
            collective_id=0, has_side_effects=True, vmem_limit_bytes=56 * 1024 * 1024
        ),
    )(trial.T, coulomb_factors, occ_values, vir_values, kernel, live_points)
    result = energy_gap[:, None] * trial.astype(f32) + total.T
    return result.astype(bf16)


def fits(mesh):
    def check(trial, coulomb_factors, occ_values, vir_values):
        return (
            mesh.shape["grp"] == 2
            and mesh.shape["vec"] == 2
            and mesh.shape["blk"] % 4 == 0
            and mesh.shape["blk"] & (mesh.shape["blk"] - 1) == 0
            and trial.shape[0] % LANES == 0
            and coulomb_factors.shape[0] % (4 * LANES) == 0
            and occ_values.shape[2] % (4 * LANES) == 0
            and occ_values.shape[1] % mesh.shape["blk"] == 0
            and vir_values.shape[2] % LANES == 0
        )

    return check


def solution(mesh):
    in_specs = (
        P(("grp", "blk", "vec"), None),
        P(("grp", "blk", "vec")),
        P("blk", None),
        P("blk", None, None),
        P("blk", None, None),
        P("blk", None),
        P("blk"),
    )
    out_specs = P(("grp", "blk", "vec"), None)
    check = fits(mesh)

    def local(trial, energy_gap, coulomb_factors, occ_values, vir_values, kernel, live_points):
        args = (trial, energy_gap, coulomb_factors, occ_values, vir_values, kernel, live_points)
        if check(trial, coulomb_factors, occ_values, vir_values):
            return fused_local(mesh.shape["blk"], *args)
        return collective_local(*args)

    return jax.shard_map(local, mesh=mesh, in_specs=in_specs, out_specs=out_specs, check_vma=False)
```

```python
import functools

import jax
import jax.numpy as jnp
from jax import lax
from jax.experimental import pallas as pl
from jax.experimental.pallas import tpu as pltpu
from jax.sharding import PartitionSpec as P

LANES = 128
MESH = pl.DeviceIdType.MESH


def collective_local(
    trial, energy_gap, coulomb_factors, occ_values, vir_values, kernel, live_points
):
    pair_rows = lax.all_to_all(trial, "vec", split_axis=1, concat_axis=0, tiled=True)
    full = lax.all_gather(pair_rows, ("grp", "blk"), axis=0, tiled=True)
    occ_count = occ_values.shape[1]
    batch_size = occ_values.shape[2]
    vir_count = vir_values.shape[2]
    width = full.shape[1]
    batches = occ_values.shape[0]
    rearranged = (
        full.reshape(occ_count, vir_count, width)
        .transpose(1, 0, 2)
        .reshape(vir_count, occ_count * width)
    )
    slots = jnp.arange(batch_size, dtype=jnp.int32)

    def coulomb_term():
        factored = jnp.dot(coulomb_factors, full, preferred_element_type=jnp.float32).astype(
            jnp.bfloat16
        )
        return 2.0 * lax.dot_general(
            coulomb_factors, factored, (((0,), (0,)), ((), ())), preferred_element_type=jnp.float32
        )

    def grid_term(first, last):

        def step(carry, items):
            occ, vir, weight, live = items
            trans = jnp.dot(vir, rearranged, preferred_element_type=jnp.float32).reshape(
                batch_size, occ_count, width
            )
            occ_float = occ.astype(jnp.float32)
            density = jnp.einsum("gik,ig->gk", trans, occ_float)
            mask = (slots < live).astype(jnp.float32)
            weighted = density * (weight * mask)[:, None]
            scaled = (
                (occ_float.T[:, :, None] * weighted[:, None, :])
                .reshape(batch_size, occ_count * width)
                .astype(jnp.bfloat16)
            )
            return (
                carry
                + lax.dot_general(
                    vir, scaled, (((0,), (0,)), ((), ())), preferred_element_type=jnp.float32
                ),
                None,
            )

        start = jnp.zeros((vir_count, occ_count * width), jnp.float32)
        items = (
            occ_values[first:last],
            vir_values[first:last],
            kernel[first:last],
            live_points[first:last],
        )
        total, _ = lax.scan(step, start, items)
        return (
            total.reshape(vir_count, occ_count, width)
            .transpose(1, 0, 2)
            .reshape(occ_count * vir_count, width)
        )

    cut = batches // 2

    def first_group():
        return coulomb_term() + grid_term(0, cut)

    def second_group():
        return grid_term(cut, batches)

    partial_sum = lax.cond(lax.axis_index("grp") == 0, first_group, second_group)
    summed = lax.psum_scatter(partial_sum, ("grp", "blk"), scatter_dimension=0, tiled=True)
    joined = lax.all_to_all(summed, "vec", split_axis=0, concat_axis=1, tiled=True)
    result = energy_gap[:, None] * trial.astype(jnp.float32) + joined
    return result.astype(jnp.bfloat16)


def fused_kernel(
    nz,
    trial_ref,
    cf_hbm,
    occ_hbm,
    vir_hbm,
    weight_ref,
    live_ref,
    out_ref,
    full,
    rear,
    cf,
    occ,
    occ_float,
    vir,
    density,
    factored,
    partial,
    land_d,
    send_a,
    land_a,
    send_b,
    land_b,
    send_z,
    land_z,
    local_sem,
    load_sem,
    gs_send,
    gs_recv,
    gd_send,
    gd_recv,
    rs_send,
    rs_recv,
    rd_send,
    rd_recv,
):
    f32, bf16 = jnp.float32, jnp.bfloat16
    _, _, chunks, width, _ = full.shape
    g, b, v = lax.axis_index("grp"), lax.axis_index("blk"), lax.axis_index("vec")
    z, y = b // 2, lax.rem(b, 2)
    g1, y1 = g + v * (1 - 2 * g), y + (1 - v) * (1 - 2 * y)
    g2, y2 = g + (1 - v) * (1 - 2 * g), y + v * (1 - 2 * y)
    g3, y3 = 1 - g, 1 - y
    kind1, kind2 = 1 + v, 2 - v
    quarter = g * 2 + v
    batches, occ_count, part = occ.shape
    vir_count = vir.shape[2]
    points = batches * part
    cf_rows = cf.shape[0]
    per_occ = vir_count // LANES
    group_occ = 4 * chunks // per_occ
    lines = group_occ * width
    step = 2 if batches % 2 == 0 else 1

    def zed(n):
        other = z
        for k in range(nz.bit_length() - 1):
            if n >> k & 1:
                other = other + (1 - 2 * lax.rem(z // 2**k, 2)) * 2**k
        return other

    def block(gg, n, yy):
        return gg * (2 * nz) + zed(n) * 2 + yy

    def at(gg, zz, yy, vv):
        return (gg, zz * 2 + yy, vv)

    p1, p2, twin = at(g1, z, y1, v), at(g2, z, y2, v), at(g, z, y, 1 - v)

    barrier = pltpu.get_barrier_semaphore()
    peers = [p1, p2, twin] + [at(g, zed(n), y, v) for n in range(1, nz)]
    for peer in peers:
        pl.semaphore_signal(barrier, inc=1, device_id=peer, device_id_type=MESH)

    own = block(g, 0, y)
    local = [
        pltpu.make_async_copy(
            trial_ref.at[:, pl.ds(c * LANES, LANES)], full.at[own, v, c], local_sem.at[c]
        )
        for c in range(chunks)
    ]
    for copy in local:
        copy.start()
    first_slot = pl.multiple_of(quarter * part, part)
    loads = [
        pltpu.make_async_copy(
            occ_hbm.at[:, :, pl.ds(first_slot, part)], occ, load_sem.at[0]
        ),
        pltpu.make_async_copy(
            vir_hbm.at[:, pl.ds(first_slot, part), :], vir, load_sem.at[1]
        ),
        pltpu.make_async_copy(
            cf_hbm.at[pl.ds(pl.multiple_of(quarter * cf_rows, cf_rows), cf_rows), :],
            cf,
            load_sem.at[2],
        ),
    ]
    for copy in loads:
        copy.start()
    for copy in local:
        copy.wait()
    pl.semaphore_wait(barrier, len(peers))

    near = list(range(1, nz))
    order = [0] + near
    sent = []

    def gather(index, j, vv, peer, send, recv):
        return pltpu.make_async_remote_copy(
            src_ref=full.at[j, vv],
            dst_ref=full.at[j, vv],
            send_sem=send.at[index],
            recv_sem=recv.at[index],
            device_id=peer,
            device_id_type=MESH,
        )

    def push(index, j, peer):
        copy = gather(index, j, v, peer, gs_send, gs_recv)
        copy.start()
        sent.append(copy)

    def push_twin(kind, n, j):
        copy = gather(kind * nz + n, j, v, twin, gd_send, gd_recv)
        copy.start()
        sent.append(copy)

    def arrive(index, j):
        gather(index, j, v, p1, gs_send, gs_recv).wait_recv()

    def from_twin(kind, n, j):
        gather(kind * nz + n, j, 1 - v, twin, gd_send, gd_recv).wait_recv()

    def absorb(gg, fx, n, slot):
        from_twin(2 * fx, n, block(gg, n, y))
        from_twin(2 * fx + 1, n, block(gg, n, y3))
        group = gg * nz + zed(n)
        for m in range(4 * chunks):
            i, c = m // per_occ, m % per_occ
            rear[slot, i * width : (i + 1) * width, c * LANES : (c + 1) * LANES] = full[
                group * 2 + m // (2 * chunks), (m // chunks) % 2, m % chunks
            ]
        for t in range(0, batches, step):
            span = slice(t * part, (t + step) * part)
            trans = lax.dot_general(
                rear[slot],
                vir[t : t + step].reshape(step * part, vir_count),
                (((1,), (1,)), ((), ())),
                preferred_element_type=f32,
            )
            o = occ_float[group, :, span]
            term = jnp.sum(trans.reshape(group_occ, width, step * part) * o[:, None, :], axis=0)
            density[:, span] = term if slot == 0 else density[:, span] + term
        total = None
        for i in range(group_occ):
            start = pl.multiple_of((group * group_occ + i) * vir_count, vir_count)
            term = lax.dot_general(
                rear[slot, i * width : (i + 1) * width, :],
                cf[:, pl.ds(start, vir_count)],
                (((1,), (1,)), ((), ())),
                preferred_element_type=f32,
            )
            total = term if total is None else total + term
        factored[...] = total if slot == 0 else factored[...] + total

    base1, base2 = nz, 2 * nz
    for n in near:
        push(n, own, at(g, zed(n), y, v))
    push(base1, own, p1)
    push(base2, own, p2)
    push_twin(0, 0, own)
    loads[0].wait()
    for k in range(2 * nz):
        for t in range(batches):
            occ_float[k, :, t * part : (t + 1) * part] = occ[
                t, k * group_occ : (k + 1) * group_occ, :
            ].astype(f32)

    def second(n):
        j = block(g1, n, y1)
        arrive(base1 + n, j)
        push(base2 + nz + n, j, p2)
        push_twin(kind1, n, j)
        j = block(g2, n, y2)
        arrive(base2 + n, j)
        push_twin(kind2, n, j)

    second(0)
    for n in near:
        j = block(g, n, y)
        arrive(n, j)
        push(base1 + n, j, p1)
        push(base2 + n, j, p2)
        push_twin(0, n, j)
    loads[1].wait()
    loads[2].wait()
    for k, n in enumerate(order):
        if k > 0:
            second(n)
            absorb(g, 0, order[k - 1], k - 1)
    for k, n in enumerate(order):
        j = block(g3, n, y3)
        arrive(base2 + nz + n, j)
        push_twin(3, n, j)
        if k == 0:
            absorb(g, 0, order[-1], nz - 1)
        else:
            absorb(g3, 1, order[k - 1], nz + k - 1)
    absorb(g3, 1, order[-1], 2 * nz - 1)

    weights = weight_ref[:, pl.ds(first_slot, part)]
    place = first_slot + lax.broadcasted_iota(jnp.int32, (1, part), 1)
    for t in range(batches):
        span = slice(t * part, (t + 1) * part)
        weight = jnp.where(place < live_ref[t], weights[t : t + 1, :], 0.0)
        density[:, span] = density[:, span] * weight
    doubled = (2.0 * factored[...].astype(bf16).astype(f32)).astype(bf16)

    def terms(gg, n):
        group = gg * nz + zed(n)
        pieces = []
        for t in range(batches):
            span = slice(t * part, (t + 1) * part)
            o = occ_float[group, :, span]
            pieces.append(
                (o[:, None, :] * density[:, span][None, :, :]).reshape(lines, part).astype(bf16)
            )
        exchange = jnp.dot(
            jnp.concatenate(pieces, axis=1),
            vir[...].reshape(points, vir_count),
            preferred_element_type=f32,
        )
        for i in range(group_occ):
            start = pl.multiple_of((group * group_occ + i) * vir_count, vir_count)
            both = exchange[i * width : (i + 1) * width, :] + jnp.dot(
                doubled, cf[:, pl.ds(start, vir_count)], preferred_element_type=f32
            )
            for c in range(per_occ):
                m = i * per_occ + c
                partial[group * 2 + m // (2 * chunks), (m // chunks) % 2, m % chunks] = both[
                    :, c * LANES : (c + 1) * LANES
                ]

    last_own = near + [0]
    drain = []

    def twin_copy(kind, n, j, vv):
        return pltpu.make_async_remote_copy(
            src_ref=partial.at[j, vv],
            dst_ref=land_d.at[j],
            send_sem=rd_send.at[kind * nz + n],
            recv_sem=rd_recv.at[kind * nz + n],
            device_id=twin,
            device_id_type=MESH,
        )

    def wire(src, dst, slot, index, peer):
        return pltpu.make_async_remote_copy(
            src_ref=src.at[slot],
            dst_ref=dst.at[slot],
            send_sem=rs_send.at[index],
            recv_sem=rs_recv.at[index],
            device_id=peer,
            device_id_type=MESH,
        )

    def pair_sum(kind, n, j):
        twin_copy(kind, n, j, 1 - v).wait_recv()
        return partial[j, v] + land_d[j]

    def give(copy):
        copy.start()
        drain.append(copy)

    def stage_a(n):
        for half, (kind, gg, yy) in enumerate(((3, g3, y3), (kind2, g2, y2))):
            k = half * nz + n
            send_a[k] = pair_sum(kind, n, block(gg, n, yy)).astype(bf16)
            give(wire(send_a, land_a, k, k, p2))

    def stage_b(n):
        total = pair_sum(kind1, n, block(g1, n, y1))
        wire(send_a, land_a, n, n, p2).wait_recv()
        send_b[n] = (total + land_a[n].astype(f32)).astype(bf16)
        give(wire(send_b, land_b, n, 2 * nz + n, p1))

    for k, n in enumerate(last_own):
        for fx, gg in ((1, g3), (0, g)):
            terms(gg, n)
            for fy, yy in ((1, y3), (0, y)):
                give(twin_copy(2 * fx + fy, n, block(gg, n, yy), 1 - v))
            if fx == 1 and k > 0:
                stage_a(last_own[k - 1])
            if fx == 0 and k > 1:
                stage_b(last_own[k - 2])
    stage_a(last_own[-1])
    for n in last_own[-2:]:
        stage_b(n)
    for n in last_own:
        total = pair_sum(0, n, block(g, n, y))
        wire(send_a, land_a, nz + n, nz + n, p2).wait_recv()
        total = total + land_a[nz + n].astype(f32)
        wire(send_b, land_b, n, 2 * nz + n, p1).wait_recv()
        total = total + land_b[n].astype(f32)
        if n > 0:
            send_z[n - 1] = total.astype(bf16)
            give(wire(send_z, land_z, n - 1, 3 * nz + n, at(g, zed(n), y, v)))
    for n in near:
        wire(send_z, land_z, n - 1, 3 * nz + n, p1).wait_recv()
        total = total + land_z[n - 1].astype(f32)
    for c in range(chunks):
        out_ref[:, c * LANES : (c + 1) * LANES] = total[c]
    for copy in sent + drain:
        copy.wait_send()


def fused_local(
    blk, trial, energy_gap, coulomb_factors, occ_values, vir_values, kernel, live_points
):
    pairs, width = trial.shape
    blocks = 2 * blk
    nz = blk // 2
    chunks = pairs // LANES
    batches, occ_count, batch_size = occ_values.shape
    vir_count = vir_values.shape[2]
    part = batch_size // 4
    cf_rows = coulomb_factors.shape[0] // 4
    group_occ = occ_count // blk
    bf16, f32 = jnp.bfloat16, jnp.float32
    vmem = pl.BlockSpec(memory_space=pltpu.VMEM)
    anywhere = pl.BlockSpec(memory_space=pl.ANY)
    dma = pltpu.SemaphoreType.DMA
    total = pl.pallas_call(
        functools.partial(fused_kernel, nz),
        out_shape=jax.ShapeDtypeStruct((width, pairs), f32),
        in_specs=[
            anywhere,
            anywhere,
            anywhere,
            anywhere,
            vmem,
            pl.BlockSpec(memory_space=pltpu.SMEM),
        ],
        out_specs=vmem,
        scratch_shapes=[
            pltpu.VMEM((blocks, 2, chunks, width, LANES), bf16),
            pltpu.VMEM((2 * nz, group_occ * width, vir_count), bf16),
            pltpu.VMEM((cf_rows, coulomb_factors.shape[1]), bf16),
            pltpu.VMEM((batches, occ_count, part), bf16),
            pltpu.VMEM((2 * nz, group_occ, batches * part), f32),
            pltpu.VMEM((batches, part, vir_count), bf16),
            pltpu.VMEM((width, batches * part), f32),
            pltpu.VMEM((width, cf_rows), f32),
            pltpu.VMEM((blocks, 2, chunks, width, LANES), f32),
            pltpu.VMEM((blocks, chunks, width, LANES), f32),
            pltpu.VMEM((2 * nz, chunks, width, LANES), bf16),
            pltpu.VMEM((2 * nz, chunks, width, LANES), bf16),
            pltpu.VMEM((nz, chunks, width, LANES), bf16),
            pltpu.VMEM((nz, chunks, width, LANES), bf16),
            pltpu.VMEM((nz, chunks, width, LANES), bf16),
            pltpu.VMEM((nz, chunks, width, LANES), bf16),
            dma((chunks,)),
            dma((3,)),
            dma((4 * nz,)),
            dma((4 * nz,)),
            dma((4 * nz,)),
            dma((4 * nz,)),
            dma((4 * nz,)),
            dma((4 * nz,)),
            dma((4 * nz,)),
            dma((4 * nz,)),
        ],
        compiler_params=pltpu.CompilerParams(
            collective_id=0, has_side_effects=True, vmem_limit_bytes=56 * 1024 * 1024
        ),
    )(trial.T, coulomb_factors, occ_values, vir_values, kernel, live_points)
    result = energy_gap[:, None] * trial.astype(f32) + total.T
    return result.astype(bf16)


def fits(mesh):
    def check(trial, coulomb_factors, occ_values, vir_values):
        return (
            mesh.shape["grp"] == 2
            and mesh.shape["vec"] == 2
            and mesh.shape["blk"] % 4 == 0
            and mesh.shape["blk"] & (mesh.shape["blk"] - 1) == 0
            and trial.shape[0] % LANES == 0
            and coulomb_factors.shape[0] % (4 * LANES) == 0
            and occ_values.shape[2] % (4 * LANES) == 0
            and occ_values.shape[1] % mesh.shape["blk"] == 0
            and vir_values.shape[2] % LANES == 0
        )

    return check


def solution(mesh):
    in_specs = (
        P(("grp", "blk", "vec"), None),
        P(("grp", "blk", "vec")),
        P("blk", None),
        P("blk", None, None),
        P("blk", None, None),
        P("blk", None),
        P("blk"),
    )
    out_specs = P(("grp", "blk", "vec"), None)
    check = fits(mesh)

    def local(trial, energy_gap, coulomb_factors, occ_values, vir_values, kernel, live_points):
        args = (trial, energy_gap, coulomb_factors, occ_values, vir_values, kernel, live_points)
        if check(trial, coulomb_factors, occ_values, vir_values):
            return fused_local(mesh.shape["blk"], *args)
        return collective_local(*args)

    return jax.shard_map(local, mesh=mesh, in_specs=in_specs, out_specs=out_specs, check_vma=False)
```
